32 devices in a mesh: dp: 8 (over z, y), mp: 4 (over x, core).
Axes of the slice: x: 2, y: 2, z: 4, core: 2. Of those that a mesh axis runs over, the one named last changes fastest.
Arguments:
- queries: bfloat16 [4096, 4096], P('dp', 'mp'), may hold values from -6 to 6
- passages: bfloat16 [4096, 4096], P('dp', 'mp'), may hold values from -6 to 6
- labels: int32 [4096], P('dp'), may hold values from 0 to 4095
- projection: bfloat16 [4096, 128], P('mp'), may hold values from -0.09375 to 0.09375
Outputs:
- loss: float32 [4096], P('dp')
- query_embed: bfloat16 [4096, 128], P('dp')
The draws below stay inside these ranges and needn't reach their ends.
All inputs are finite; a program needn't handle non-finite values.
Results may differ from the reference program's by a relative error of at most 0.0039.
Values may be sent and summed in bfloat16 or wider, within the bound.
No kernel may reach another device: no remote copies, remote signals or barrier semaphores. Data moves between devices by JAX's collectives and lax.ppermute only.
A program may use at most 64 MiB of HBM per device.

```python
import jax
import jax.numpy as jnp
from jax import lax

D = 4096
E = 128
BATCH = 4096


def draw_states(key, salt):
    subkey = jax.random.fold_in(key, salt)
    values = jnp.clip(jax.random.normal(subkey, (BATCH, D), jnp.float32), -6.0, 6.0)
    return values


def draw_passages(key, part):
    return draw_states(key, 11).astype(jnp.bfloat16)


def draw_queries(key, part):
    values = draw_states(key, 7)
    return values.astype(jnp.bfloat16)


def set_ends(values, key, smallest, largest):
    spot = [jax.random.randint(jax.random.fold_in(key, axis), (), 0, length) for axis, length in enumerate(values.shape)]
    main_axis = values.shape.index(max(values.shape))
    neighbour = spot[:main_axis] + [(spot[main_axis] + 1) % values.shape[main_axis]] + spot[main_axis + 1:]
    return values.at[tuple(spot)].set(smallest).at[tuple(neighbour)].set(largest)


def block_levels(own_key, dims, split, smallest, high):
    factor_of, own = 1.0, jax.random.fold_in(own_key, 6)
    for position, blocks in split:
        heights = jnp.exp(jax.random.uniform(jax.random.fold_in(own, position), (blocks,), jnp.float32, smallest / len(split), high / len(split)))
        factor_of = factor_of * jnp.repeat(heights, dims[position] // blocks).reshape([-1 if axis == position else 1 for axis in range(len(dims))])
    return factor_of


def normal_values(stream_key, extent, width, reach, shards=(), kind=jnp.bfloat16):
    drawn = jax.random.normal(stream_key, extent, jnp.float32) * width
    if len(shards) > 0:
        drawn = block_levels(stream_key, extent, shards, -0.22, 0.18) * drawn
    return jnp.clip(drawn, min=-reach, max=reach).astype(kind)


def setup_inputs(seed: int = 0) -> dict:
    keys = jax.random.split(jax.random.key(seed), 5)
    queries = draw_queries(jax.random.fold_in(keys[4], 71), 0)
    passages = draw_passages(jax.random.fold_in(keys[4], 71), 0)
    labels = set_ends(jax.random.randint(keys[2], (BATCH,), 0, BATCH), jax.random.fold_in(keys[2], 1), 0, BATCH - 1).astype(jnp.int32)
    projection = normal_values(keys[3], (D, E), D ** -0.5, 0.09375, ((0, 4),))
    return {"queries": queries, "passages": passages, "labels": labels, "projection": projection}


def reference(queries, passages, labels, projection):
    query_embed = jnp.dot(queries, projection, preferred_element_type=jnp.float32).astype(jnp.bfloat16)
    passage_embed = jnp.dot(passages, projection, preferred_element_type=jnp.float32).astype(jnp.bfloat16)
    block = min(512, BATCH)
    count = BATCH // block
    query_blocks = query_embed.reshape(count, block, E)
    label_blocks = labels.reshape(count, block)

    def one_block(args):
        qblock, lblock = args
        scores = jnp.dot(qblock, passage_embed.T, preferred_element_type=jnp.float32)
        total = jax.nn.logsumexp(scores, axis=1)
        chosen = jnp.take_along_axis(scores, lblock[:, None].astype(jnp.int32), axis=1)[:, 0]
        return total - chosen

    loss = lax.map(one_block, (query_blocks, label_blocks)).reshape(BATCH)
    return loss, query_embed
```

```python
import jax
import jax.numpy as jnp
from jax import lax
from jax.sharding import PartitionSpec as P

AXES = ("dp", "mp")


def swap(value, dp_bits, mp_bits):
    dp, mp = lax.axis_size("dp"), lax.axis_size("mp")
    pairs = [
        (d * mp + m, (d ^ dp_bits) * mp + (m ^ mp_bits)) for d in range(dp) for m in range(mp)
    ]
    return lax.ppermute(value, AXES, pairs)


def half(value, index):
    size = value.shape[0] // 2
    return lax.dynamic_slice_in_dim(value, index * size, size, 0)


def joined(mine, other, index):
    return jnp.where(
        index == 0,
        jnp.concatenate([mine, other], axis=0),
        jnp.concatenate([other, mine], axis=0),
    )


def split_pair(value):
    high = value.astype(jnp.bfloat16)
    low = (value - high.astype(jnp.float32)).astype(jnp.bfloat16)
    return jnp.concatenate([high, low], axis=0)


def pair_sum(pair):
    size = pair.shape[0] // 2
    return pair[:size].astype(jnp.float32) + pair[size:].astype(jnp.float32)


def statistics(scores, hit):
    top = jnp.max(scores, axis=0)
    total = jnp.sum(jnp.exp(scores - top[None, :]), axis=0)
    chosen = jnp.sum(jnp.where(hit, scores, 0.0), axis=0)
    return jnp.stack([top, total, chosen])


def bit_groups(dp):
    bits = []
    bit = dp // 4
    while bit:
        bits.append(bit)
        bit //= 2
    return [bits[i : i + 2] for i in range(0, len(bits), 2)]


def per_device(queries, passages, labels, projection):
    rows = queries.shape[0]
    dp = lax.axis_size("dp")
    group, member = lax.axis_index("dp"), lax.axis_index("mp")
    inner, outer = member % 2, member // 2

    passage_part = jnp.dot(passages, projection, preferred_element_type=jnp.float32)
    query_part = jnp.dot(queries, projection, preferred_element_type=jnp.float32)

    passage_half = half(passage_part, inner) + swap(half(passage_part, 1 - inner), 0, 1)
    query_half = half(query_part, inner) + swap(half(query_part, 1 - inner), 0, 1)

    passage_half = passage_half.astype(jnp.bfloat16)
    near, far = half(passage_half, outer), half(passage_half, 1 - outer)
    top_bit = dp // 2
    got_outer = swap(far, 0, 2)
    got_top = swap(near, top_bit, 0)
    got_both = swap(far, top_bit, 2)
    query_pair = split_pair(query_half)
    query_sum = pair_sum(query_pair) + pair_sum(swap(query_pair, 0, 2))
    query_mine = query_sum.astype(jnp.bfloat16)
    query_embed = joined(query_mine, swap(query_mine, 0, 1), inner)

    def added(first, second):
        return (first.astype(jnp.float32) + second.astype(jnp.float32)).astype(jnp.bfloat16)

    held = jnp.stack([added(near, got_outer), added(got_top, got_both)])
    offsets = [0, top_bit]
    for bits in bit_groups(dp):
        moves = [bits[0], bits[1], bits[0] ^ bits[1]] if len(bits) == 2 else [bits[0]]
        held = jnp.concatenate([held] + [swap(held, move, 0) for move in moves], axis=0)
        offsets = offsets + [offset ^ move for move in moves for offset in offsets]

    quarter = rows // 4
    first = (inner * 2 + outer) * quarter
    starts = (group ^ jnp.array(offsets, jnp.int32)) * rows + first
    ids = (starts[:, None] + jnp.arange(quarter, dtype=jnp.int32)[None, :]).reshape(-1)
    block = held.reshape(-1, held.shape[-1])
    scores = lax.dot_general(
        block, query_embed, (((1,), (1,)), ((), ())), preferred_element_type=jnp.float32
    )
    mine = statistics(scores, ids[:, None] == labels[None, :])
    parts = [mine, swap(mine, 0, 1), swap(mine, 0, 2), swap(mine, 0, 3)]
    top = jnp.maximum(
        jnp.maximum(parts[0][0], parts[1][0]), jnp.maximum(parts[2][0], parts[3][0])
    )
    terms = [part[1] * jnp.exp(part[0] - top) for part in parts]
    total = (terms[0] + terms[1]) + (terms[2] + terms[3])
    chosen = (parts[0][2] + parts[1][2]) + (parts[2][2] + parts[3][2])
    loss = top + jnp.log(total) - chosen
    return (loss, query_embed)


def solution(mesh):
    return jax.shard_map(
        per_device,
        mesh=mesh,
        in_specs=(P("dp", "mp"), P("dp", "mp"), P("dp"), P("mp", None)),
        out_specs=(P("dp"), P("dp", None)),
        check_vma=False,
    )
```

```python
import jax
import jax.numpy as jnp
from jax import lax
from jax.experimental import pallas as pl
from jax.experimental.pallas import tpu as pltpu
from jax.sharding import PartitionSpec as P

AXES = ("dp", "mp")


def swap(value, dp_bits, mp_bits):
    dp, mp = lax.axis_size("dp"), lax.axis_size("mp")
    pairs = [
        (d * mp + m, (d ^ dp_bits[m % 2]) * mp + (m ^ mp_bits))
        for d in range(dp)
        for m in range(mp)
    ]
    return lax.ppermute(value, AXES, pairs)


def half(value, index):
    size = value.shape[0] // 2
    return lax.dynamic_slice_in_dim(value, index * size, size, 0, allow_negative_indices=False)


def joined(mine, other, index):
    return jnp.where(
        index == 0,
        jnp.concatenate([mine, other], axis=0),
        jnp.concatenate([other, mine], axis=0),
    )


def projected(passages, queries, projection):
    rows, depth = queries.shape
    embed = projection.shape[1]
    chunks = 2
    size = rows // chunks

    def kernel(passage_hbm, query_hbm, weight_hbm, out_ref, buffer, weight, sems):
        load_weight = pltpu.make_async_copy(weight_hbm, weight, sems.at[2 * chunks])
        load_weight.start()
        loads = []
        for c in range(chunks):
            for which, source in enumerate((passage_hbm, query_hbm)):
                loads.append(
                    pltpu.make_async_copy(
                        source.at[pl.ds(c * size, size)],
                        buffer.at[which, pl.ds(c * size, size)],
                        sems.at[2 * c + which],
                    )
                )
                loads[-1].start()
        load_weight.wait()
        for c in range(chunks):
            for which in range(2):
                loads[2 * c + which].wait()
                sums = jnp.dot(
                    buffer[which, c * size : (c + 1) * size],
                    weight[...],
                    preferred_element_type=jnp.float32,
                )
                side, start = divmod(c * size, rows // 2)
                if size <= rows // 2:
                    out_ref[side, which, start : start + size] = sums
                else:
                    out_ref[0, which] = sums[: rows // 2]
                    out_ref[1, which] = sums[rows // 2 :]

    return pl.pallas_call(
        kernel,
        in_specs=[pl.BlockSpec(memory_space=pl.ANY)] * 3,
        out_specs=pl.BlockSpec(memory_space=pltpu.VMEM),
        out_shape=pltpu.VMEM((2, 2, rows // 2, embed), jnp.float32),
        scratch_shapes=[
            pltpu.VMEM((2, rows, depth), queries.dtype),
            pltpu.VMEM((depth, embed), projection.dtype),
            pltpu.SemaphoreType.DMA((2 * chunks + 1,)),
        ],
    )(passages, queries, projection)


def statistics(scores, hit):
    top = jnp.max(scores, axis=0)
    total = jnp.sum(jnp.exp(scores - top[None, :]), axis=0)
    chosen = jnp.sum(jnp.where(hit, scores, 0.0), axis=0)
    return jnp.stack([top, total, chosen])


def last_moves(dp):
    if dp >= 8:
        return [(1, 5), (2, 4), (3, 7)], 6
    if dp == 4:
        return [(1, 2)], 3
    return [], dp - 1


def early_moves(dp):
    bits = []
    bit = dp // 2
    while bit >= 8:
        bits.append(bit)
        bit //= 2
    return bits


def per_device(queries, passages, labels, projection):
    rows = queries.shape[0]
    size, quarter = rows // 2, rows // 4
    dp = lax.axis_size("dp")
    group, member = lax.axis_index("dp"), lax.axis_index("mp")
    inner, outer = member & 1, member >> 1

    parts = projected(passages, queries, projection)
    query_sent = lax.dynamic_index_in_dim(parts[:, 1], 1 - inner, 0, False, allow_negative_indices=False)
    query_kept = lax.dynamic_index_in_dim(parts[:, 1], inner, 0, False, allow_negative_indices=False)
    passage_part = parts[:, 0].reshape(rows, -1)
    met = swap(jnp.concatenate([passage_part, query_sent], axis=0), (0, 0), 1)
    passage_chip = passage_part + met[:rows]
    query_chip = query_kept + met[rows:]

    far = half(passage_chip, 1 - outer).astype(jnp.bfloat16)
    got = swap(far, (0, 0), 2)
    block = (half(passage_chip, outer) + got.astype(jnp.float32)).astype(jnp.bfloat16)
    query_sum = query_chip + swap(query_chip, (0, 0), 2)
    query_mine = query_sum.astype(jnp.bfloat16)
    query_embed = joined(query_mine, swap(query_mine, (0, 0), 1), inner)

    held, offsets = block[None], [0]
    for bit in early_moves(dp):
        held = jnp.concatenate([held, swap(held, (bit, bit), 0)], axis=0)
        offsets = offsets + [offset ^ bit for offset in offsets]

    def own_half(value):
        return lax.dynamic_slice_in_dim(
            value, inner * quarter, quarter, 1, allow_negative_indices=False
        )

    pairs, shared = last_moves(dp)
    pieces, starts = [own_half(held)], [(0, inner * quarter, quarter)]
    for even, odd in pairs:
        pieces.append(swap(held, (even, odd), 0))
        starts.append((jnp.where(inner == 0, even, odd), 0, size))
    if shared:
        pieces.append(swap(own_half(held), (shared, shared), 0))
        starts.append((shared, inner * quarter, quarter))
    ids = jnp.concatenate(
        [
            (group ^ offset ^ move) * rows
            + outer * size
            + begin
            + jnp.arange(length, dtype=jnp.int32)
            for move, begin, length in starts
            for offset in offsets
        ]
    )
    passage_block = jnp.concatenate(
        [piece.reshape(-1, piece.shape[-1]) for piece in pieces], axis=0
    )
    scores = lax.dot_general(
        passage_block, query_embed, (((1,), (1,)), ((), ())), preferred_element_type=jnp.float32
    )
    mine = statistics(scores, ids[:, None] == labels[None, :])
    parts = [mine] + [swap(mine, (0, 0), bits) for bits in (1, 2, 3)]
    top = jnp.maximum(
        jnp.maximum(parts[0][0], parts[1][0]), jnp.maximum(parts[2][0], parts[3][0])
    )
    terms = [part[1] * jnp.exp(part[0] - top) for part in parts]
    total = (terms[0] + terms[1]) + (terms[2] + terms[3])
    chosen = (parts[0][2] + parts[1][2]) + (parts[2][2] + parts[3][2])
    loss = top + jnp.log(total) - chosen
    return (loss, query_embed)


def solution(mesh):
    return jax.shard_map(
        per_device,
        mesh=mesh,
        in_specs=(P("dp", "mp"), P("dp", "mp"), P("dp"), P("mp", None)),
        out_specs=(P("dp"), P("dp", None)),
        check_vma=False,
    )
```

```python
import jax
import jax.numpy as jnp
from jax import lax
from jax.experimental import pallas as pl
from jax.experimental.pallas import tpu as pltpu
from jax.sharding import PartitionSpec as P

AXES = ("dp", "mp")


def swap(name, value, dp_bits, mp_bits):
    dp, mp = lax.axis_size("dp"), lax.axis_size("mp")
    pairs = [
        (d * mp + m, (d ^ dp_bits[m % 2]) * mp + (m ^ mp_bits))
        for d in range(dp)
        for m in range(mp)
    ]
    with jax.named_scope(name):
        return lax.ppermute(value, AXES, pairs)


def half(value, index):
    size = value.shape[0] // 2
    return lax.dynamic_slice_in_dim(value, index * size, size, 0, allow_negative_indices=False)


def project(states, projection):
    rows, depth = states.shape
    embed = projection.shape[1]
    size = rows // 2

    def kernel(states_hbm, weight_hbm, out, buffer, weight, sems):
        copies = [pltpu.make_async_copy(weight_hbm, weight, sems.at[0])]
        for c in range(2):
            part = pl.ds(c * size, size)
            copies.append(
                pltpu.make_async_copy(states_hbm.at[part], buffer.at[part], sems.at[1 + c])
            )
        for copy in copies:
            copy.start()
        copies[0].wait()
        for c in range(2):
            copies[1 + c].wait()
            part = slice(c * size, (c + 1) * size)
            out[part] = jnp.dot(buffer[part], weight[...], preferred_element_type=jnp.float32)

    return pl.pallas_call(
        kernel,
        in_specs=[pl.BlockSpec(memory_space=pl.ANY)] * 2,
        out_specs=pl.BlockSpec(memory_space=pltpu.VMEM),
        out_shape=pltpu.VMEM((rows, embed), jnp.float32),
        scratch_shapes=[
            pltpu.VMEM((rows, depth), states.dtype),
            pltpu.VMEM((depth, embed), projection.dtype),
            pltpu.SemaphoreType.DMA((3,)),
        ],
    )(states, projection)


def statistics(passages, ids, queries, labels):
    scores = lax.dot_general(
        passages, queries, (((1,), (1,)), ((), ())), preferred_element_type=jnp.float32
    )
    top = jnp.max(scores, axis=0)
    total = jnp.sum(jnp.exp(scores - top[None, :]), axis=0)
    chosen = jnp.sum(jnp.where(ids[:, None] == labels[None, :], scores, 0.0), axis=0)
    return jnp.stack([top, total, chosen])


def merged(first, second):
    top = jnp.maximum(first[0], second[0])
    total = first[1] * jnp.exp(first[0] - top) + second[1] * jnp.exp(second[0] - top)
    return jnp.stack([top, total, first[2] + second[2]])


def last_moves(dp):
    if dp >= 8:
        return [(4, 5), (6, 7), (1, 1), (2, 3)]
    if dp == 4:
        return [(1, 2), (3, 3)]
    return [(1, 1)] if dp == 2 else []


def early_moves(dp):
    bits = []
    bit = dp // 2
    while bit >= 8:
        bits.append(bit)
        bit //= 2
    return bits


def per_device(queries, passages, labels, projection):
    rows = queries.shape[0]
    size, quarter = rows // 2, rows // 4
    dp = lax.axis_size("dp")
    group, member = lax.axis_index("dp"), lax.axis_index("mp")
    inner, outer = member & 1, member >> 1

    with jax.named_scope("project_p"):
        passage_part = project(passages, projection)
    far = half(passage_part, 1 - outer).astype(jnp.bfloat16)
    passage_sum = half(passage_part, outer) + swap("passage_far", far, (0, 0), 2).astype(jnp.float32)
    passage_sum = passage_sum + swap("passage_core", passage_sum, (0, 0), 1)
    block = passage_sum.astype(jnp.bfloat16)

    with jax.named_scope("project_q"):
        query_part = project(queries, projection)
    query_sum = query_part + swap("query_far", query_part, (0, 0), 2)
    query_embed = (query_sum + swap("query_core", query_sum, (0, 0), 1)).astype(jnp.bfloat16)

    held, offsets = block[None], [0]
    for bit in early_moves(dp):
        held = jnp.concatenate([held, swap("early", held, (bit, bit), 0)], axis=0)
        offsets = offsets + [offset ^ bit for offset in offsets]

    def own_half(value):
        return lax.dynamic_slice_in_dim(
            value, inner * quarter, quarter, 1, allow_negative_indices=False
        )

    def taken(pieces):
        blocks, ids = [], []
        for piece, move, begin in pieces:
            blocks.append(piece.reshape(-1, piece.shape[-1]))
            span = jnp.arange(piece.shape[1], dtype=jnp.int32)
            for offset in offsets:
                ids.append((group ^ offset ^ move) * rows + outer * size + begin + span)
        return statistics(
            jnp.concatenate(blocks, axis=0), jnp.concatenate(ids), query_embed, labels
        )

    pieces = [(own_half(held), 0, inner * quarter)]
    for i, (even, odd) in enumerate(last_moves(dp)):
        if even == odd:
            got = swap(f"gather{i}", own_half(held), (even, even), 0)
            pieces.append((got, even, inner * quarter))
        else:
            got = swap(f"gather{i}", held, (even, odd), 0)
            pieces.append((got, jnp.where(inner == 0, even, odd), 0))
    mine = taken(pieces)
    with jax.named_scope("merge"):
        mine = merged(mine, swap("stat_core", mine, (0, 0), 1))
        top, total, chosen = merged(mine, swap("stat_far", mine, (0, 0), 3))
        loss = top + jnp.log(total) - chosen
    return (loss, query_embed)


def solution(mesh):
    return jax.shard_map(
        per_device,
        mesh=mesh,
        in_specs=(P("dp", "mp"), P("dp", "mp"), P("dp"), P("mp", None)),
        out_specs=(P("dp"), P("dp", None)),
        check_vma=False,
    )
```
